32 devices in a mesh: sec: 2 (over y), tp: 4 (over x, core), dp: 4 (over z).
Axes of the slice: x: 2, y: 2, z: 4, core: 2. Of those that a mesh axis runs over, the one named last changes fastest.
Arguments:
- feats: bfloat16 [8, 512, 512], P(('sec', 'dp'), 'tp'), may hold values from -6 to 6
- frame_clip: int32 [8, 32], P(('sec', 'dp')), may hold values from 0 to 3, never falling along the last dimension, each value on 1 to 16 neighbouring positions
- clip_order: int32 [8, 4], P(('sec', 'dp')), may hold values from 0 to 3, each once within a row
- conv_weight: bfloat16 [3, 512, 192], replicated, may hold values from -0.15625 to 0.15625
- embed_weight: bfloat16 [192, 3072], replicated, may hold values from -0.4375 to 0.4375
- wq: bfloat16 [3072, 512], P(('sec', 'dp'), 'tp')
- wk: bfloat16 [3072, 512], P(('sec', 'dp'), 'tp')
- wv: bfloat16 [3072, 512], P(('sec', 'dp'), 'tp'), may hold values from -0.109375 to 0.109375
- q_gain: float32 [4, 128], P('tp'), may hold values from 0.6 to 8, as said below
- k_gain: float32 [4, 128], P('tp'), may hold values from 0.6 to 8, as said below
Outputs:
- attended: bfloat16 [8, 512, 512], P(('sec', 'dp'), 'tp')
The draws below stay inside these ranges and needn't reach their ends.
Inputs may be any that keep to these rules, and one draw needn't show every extreme that they name: `frame_clip`: clip ids never fall along the frames; every clip has at least one frame and one clip has exactly 16 frames. `clip_order`: each row holds every clip once. `q_gain`: positive. `k_gain`: positive.
All inputs are finite; a program needn't handle non-finite values.
Results may differ from the reference program's by a relative error of at most 0.0084.
Values may be sent and summed in bfloat16 or wider, within the bound.
A program may use at most 64 MiB of HBM per device.

```python
import math
import jax
import jax.numpy as jnp
import numpy as np
from jax import lax

D = 3072
HD = 128
PD = 192
FIN = 512
TAPS = 3
VP = 16
CLIPS = 4
HEADS = 4
NF = 32
S = 512
BUCKETS = 8


def shared_projection(key, salt):
    own_part = jax.random.normal(jax.random.fold_in(key, salt), (D, HEADS * HD), jnp.float32)
    return own_part * D ** (-0.5)


def gain_values(key, salt):
    uniform_part = jax.random.uniform(jax.random.fold_in(key, salt), (HEADS, HD), jnp.float32)
    lower, upper = (0.6, 1.6)
    return jnp.exp(jnp.log(lower) + uniform_part * (jnp.log(upper) - jnp.log(lower)))


def draw_wq(key, part):
    return shared_projection(key, 3).astype(jnp.bfloat16)


def draw_wk(key, part):
    return shared_projection(key, 5).astype(jnp.bfloat16)


def draw_q_gain(key, part):
    return gain_values(key, 7)


def draw_k_gain(key, part):
    return gain_values(key, 11)


def levels(stream_key, extent, shards, least, top_value):
    loudness = 1.0
    for position, parts in shards:
        heights = jax.random.uniform(jax.random.fold_in(jax.random.fold_in(stream_key, 6), position), (parts,), jnp.float32, least / len(shards), top_value / len(shards))
        loudness = loudness * jnp.repeat(jnp.exp(heights), extent[position] // parts).reshape((-1,) + (1,) * (len(extent) - 1 - position))
    return loudness


def split_up(number_of, total, bound, skew):
    portions = [(1 << 20) // math.isqrt(grade ** skew) + 1 for grade in range(2, number_of + 1)]
    surplus, counts = total - bound - (number_of - 1), [1] * (number_of - 1)
    while surplus > 0:
        movable = [i for i in range(number_of - 1) if counts[i] < bound]
        pool, budget = sum([portions[i] for i in movable]), surplus
        for i in movable:
            extra = min(bound - counts[i], max(1, budget * portions[i] // pool), surplus)
            counts[i] = counts[i] + extra
            surplus = surplus - extra
    return np.array([bound] + counts)


def uneven_parts(own_key, number_of, total, reach, skew):
    if number_of == 2:
        one = jax.random.randint(own_key, (), max(1, total - reach), min(reach, total - 1) + 1)
        return jnp.stack([one, total - one])
    tallies = jnp.asarray(split_up(number_of, total, reach, skew), jnp.int32)
    twos = (number_of - 1) // 2
    source_of, receiver = tallies[1:1 + 2 * twos:2], tallies[2:2 + 2 * twos:2]
    room = jnp.minimum(source_of - 1, reach - receiver)
    moved = jax.random.randint(jax.random.fold_in(own_key, 1), (twos,), 0, 1 << 20) % (room + 1)
    tallies = tallies.at[1:1 + 2 * twos:2].set(source_of - moved).at[2:2 + 2 * twos:2].set(receiver + moved)
    return tallies[jax.random.permutation(jax.random.fold_in(own_key, 2), number_of)]


def scatter_about(own_key, extent, scale, reach, pieces=(), kind=jnp.bfloat16):
    drawn = jax.random.normal(own_key, extent, jnp.float32) * scale
    if len(pieces) > 0:
        drawn = levels(own_key, extent, pieces, -0.22, 0.18) * drawn
    return jnp.clip(drawn, min=-reach, max=reach).astype(kind)


def setup_inputs(seed: int = 0) -> dict:
    splits = jax.random.split(jax.random.key(seed), 11)
    return {
        "feats": scatter_about(splits[0], (BUCKETS, S, FIN), 1.0, 6.0, ((0, 8), (1, 4))),
        "frame_clip": jax.vmap(lambda own: jnp.searchsorted(jnp.cumsum(uneven_parts(own, CLIPS, NF, NF // 2, 1)), jnp.arange(NF), side="right"))(jax.random.split(splits[1], BUCKETS)).reshape((BUCKETS, NF)).astype(jnp.int32),
        "clip_order": jax.vmap(lambda own: jax.random.permutation(own, CLIPS))(jax.random.split(splits[2], BUCKETS)).reshape((BUCKETS, CLIPS)).astype(jnp.int32),
        "conv_weight": scatter_about(splits[3], (TAPS, FIN, PD), (TAPS * FIN) ** -0.5, 0.15625),
        "embed_weight": scatter_about(splits[4], (PD, D), PD ** -0.5, 0.4375),
        "wq": draw_wq(jax.random.fold_in(splits[10], 71), 0),
        "wk": draw_wk(jax.random.fold_in(splits[10], 71), 0),
        "wv": scatter_about(splits[7], (D, HEADS * HD), D ** -0.5, 0.109375, ((0, 8), (1, 4))),
        "q_gain": draw_q_gain(jax.random.fold_in(splits[10], 71), 0),
        "k_gain": draw_k_gain(jax.random.fold_in(splits[10], 71), 0),
    }


def packing(clip_ids, clip_order):
    frame_count = clip_ids.shape[0]
    clip_count = clip_order.shape[0]
    labels = jnp.arange(clip_count, dtype=jnp.int32)
    lengths = lax.optimization_barrier(jnp.sum((clip_ids[None, :] == labels[:, None]).astype(jnp.int32), axis=1)).astype(jnp.int32)
    starts = (jnp.cumsum(lengths) - lengths).astype(jnp.int32)
    picked = clip_order[:, None] == labels[None, :]
    packed_len = lax.optimization_barrier(jnp.sum(jnp.where(picked, lengths[None, :], 0), axis=1)).astype(jnp.int32)
    packed_from = lax.optimization_barrier(jnp.sum(jnp.where(picked, starts[None, :], 0), axis=1)).astype(jnp.int32)
    place_start = (jnp.cumsum(packed_len) - packed_len).astype(jnp.int32)
    frames = jnp.arange(frame_count, dtype=jnp.int32)
    places = lax.optimization_barrier(jnp.sum((frames[:, None] >= place_start[None, :]).astype(jnp.int32), axis=1)).astype(jnp.int32) - 1
    chosen = places[:, None] == labels[None, :]
    source = lax.optimization_barrier(jnp.sum(jnp.where(chosen, (packed_from - place_start)[None, :], 0), axis=1)) + frames
    return (source.astype(jnp.int32), places.astype(jnp.int32))

def encode(feature, clip_ids, conv_weight):
    frame_count = clip_ids.shape[0]
    cubes = feature.reshape(frame_count, VP, FIN)
    summed = jnp.zeros((frame_count * VP, PD), jnp.float32)
    for delay in range(TAPS):
        earlier = jnp.concatenate([jnp.zeros((delay, VP, FIN), cubes.dtype), cubes[:frame_count - delay]], axis=0)
        earlier_ids = jnp.concatenate([jnp.full((delay,), -1, jnp.int32), clip_ids[:frame_count - delay].astype(jnp.int32)])
        in_clip = jnp.repeat(earlier_ids == clip_ids.astype(jnp.int32), VP)
        contrib = jnp.dot(earlier.reshape(-1, FIN), conv_weight[delay], preferred_element_type=jnp.float32)
        summed = summed + jnp.where(in_clip[:, None], contrib, 0.0)
    return summed.astype(jnp.bfloat16)

def normed(values, gains):
    scale = lax.rsqrt(lax.optimization_barrier(jnp.mean(values * values, axis=-1, keepdims=True)) + 1e-06)
    return (values * scale * gains[None, :]).astype(jnp.bfloat16)

def attend(query, key_rows, value_rows, segment):
    scores = jnp.dot(query, key_rows.T, preferred_element_type=jnp.float32) * HD ** (-0.5)
    same_seg = segment[:, None] == segment[None, :]
    scores = jnp.where(same_seg, scores, -1e+30)
    highest = lax.optimization_barrier(jnp.max(scores, axis=-1, keepdims=True))
    expo = jnp.where(same_seg, jnp.exp(scores - highest), 0.0)
    probs = (expo / lax.optimization_barrier(jnp.sum(expo, axis=-1, keepdims=True))).astype(jnp.bfloat16)
    return jnp.dot(probs, value_rows, preferred_element_type=jnp.float32).astype(jnp.bfloat16)

def reference(feats, frame_clip, clip_order, conv_weight, embed_weight, wq, wk, wv, q_gain, k_gain):

    def one_bucket(inputs):
        feature, clip_ids, order = inputs
        latent = encode(feature, clip_ids, conv_weight)
        tokens = jnp.dot(latent, embed_weight, preferred_element_type=jnp.float32).astype(jnp.bfloat16)
        source, places = packing(clip_ids, order)
        slots = (source[:, None] * VP + jnp.arange(VP, dtype=jnp.int32)[None, :]).reshape(-1)
        segment = jnp.repeat(places, VP)
        packed = jnp.take(tokens, slots, axis=0)

        def head_step(carry, head):
            begin = (head * HD).astype(jnp.int32)
            query = jnp.dot(packed, lax.dynamic_slice_in_dim(wq, begin, HD, 1), preferred_element_type=jnp.float32)
            key_raw = jnp.dot(packed, lax.dynamic_slice_in_dim(wk, begin, HD, 1), preferred_element_type=jnp.float32)
            value_raw = jnp.dot(packed, lax.dynamic_slice_in_dim(wv, begin, HD, 1), preferred_element_type=jnp.float32)
            gain_q = lax.dynamic_index_in_dim(q_gain, head, 0, keepdims=False)
            gain_k = lax.dynamic_index_in_dim(k_gain, head, 0, keepdims=False)
            mixed = attend(normed(query, gain_q), normed(key_raw, gain_k), value_raw.astype(jnp.bfloat16), segment)
            return (carry, mixed)
        _, stacked = lax.scan(head_step, jnp.zeros((), jnp.float32), jnp.arange(HEADS, dtype=jnp.int32))
        return jnp.transpose(stacked, (1, 0, 2)).reshape(S, HEADS * HD)
    return lax.map(one_bucket, (feats, frame_clip, clip_order))
```

```python
import functools
import jax
import jax.numpy as jnp
from jax import lax
from jax.experimental import pallas as pl
from jax.experimental.pallas import tpu as pltpu
from jax.sharding import PartitionSpec as P

HD = 128
VP = 16
MESH = pl.DeviceIdType.MESH
BF16 = jnp.bfloat16
F32 = jnp.float32


def dot32(a, b):
    return jnp.dot(a, b, preferred_element_type=F32)


def kernel(
    sizes, direct_embed,
    frame_ref, order_ref, feats_ref, conv_ref, embed_ref, wq_ref, wk_ref, wv_ref, gq_ref, gk_ref,
    out_ref,
    wide, conv, embed, weights, part_out, part_in, own_sum, left_in, left_out, right_in, right_out,
    latents, queries, keys, values, mixed,
    local_sem, rim_send, rim_recv, sec_send, sec_recv, dp_send, dp_recv, lat_send, lat_recv, out_send, out_recv,
):
    n_sec, n_tp, n_dp = sizes
    sec, me, dp = lax.axis_index("sec"), lax.axis_index("tp"), lax.axis_index("dp")
    rows = feats_ref.shape[0]
    taps, fin, pd = conv_ref.shape
    depth = wq_ref.shape[0]
    reach_rows = (taps - 1) * VP
    total = rows * n_tp
    frame_count = frame_ref.shape[1]
    clip_count = order_ref.shape[1]
    sec_peers = [lax.rem(sec + d, n_sec) for d in range(1, n_sec)]
    tp_peers = [lax.rem(me + d, n_tp) for d in range(1, n_tp)]

    barrier = pltpu.get_barrier_semaphore()

    def greet(where):
        pl.semaphore_signal(barrier, inc=1, device_id=where, device_id_type=MESH)

    for peer in sec_peers:
        greet({"sec": peer})
    for peer in tp_peers:
        greet({"tp": peer})

    @pl.when(dp > 0)
    def _():
        greet({"dp": dp - 1})

    @pl.when(dp < n_dp - 1)
    def _():
        greet({"dp": dp + 1})

    if direct_embed:
        begin = pl.multiple_of((sec * n_dp + dp) * depth, 128)
        embed_from = embed_ref.at[:, pl.ds(begin, depth)]
    else:
        embed_from = embed_ref
    loads = [
        pltpu.make_async_copy(embed_from, embed, local_sem.at[0]),
        pltpu.make_async_copy(wq_ref, weights.at[0], local_sem.at[1]),
        pltpu.make_async_copy(wk_ref, weights.at[1], local_sem.at[2]),
        pltpu.make_async_copy(wv_ref, weights.at[2], local_sem.at[3]),
        pltpu.make_async_copy(feats_ref, wide.at[pl.ds(reach_rows, rows)], local_sem.at[4]),
        pltpu.make_async_copy(conv_ref, conv, local_sem.at[5]),
    ]
    for load in loads:
        load.start()

    first = [jnp.int32(0) for _ in range(clip_count)]
    for f in range(frame_count):
        clip = frame_ref[0, f]
        for c in range(1, clip_count):
            first[c] = first[c] + (clip < c).astype(jnp.int32)
    lengths = [
        (first[c + 1] if c + 1 < clip_count else jnp.int32(frame_count)) - first[c]
        for c in range(clip_count)
    ]
    place_start, place_shift, place_of = [], [], [jnp.int32(0) for _ in range(clip_count)]
    running = jnp.int32(0)
    for r in range(clip_count):
        clip = order_ref[0, r]
        length, start = jnp.int32(0), jnp.int32(0)
        for c in range(clip_count):
            here = clip == c
            length = jnp.where(here, lengths[c], length)
            start = jnp.where(here, first[c], start)
            place_of[c] = jnp.where(here, r, place_of[c])
        place_start.append(running)
        place_shift.append(start - running)
        running = running + length

    def clip_at(row):
        clip = jnp.zeros_like(row)
        for c in range(1, clip_count):
            clip = clip + (row >= first[c] * VP).astype(jnp.int32)
        return clip

    for load in loads[:4]:
        load.wait()
    for c in range(3):
        partial = dot32(embed[...], weights[c])
        own_sum[c] = partial
        part_out[c] = partial.astype(BF16)

    line_peers = (dp > 0).astype(jnp.int32) + (dp < n_dp - 1).astype(jnp.int32)
    pl.semaphore_wait(barrier, (n_sec - 1) + (n_tp - 1) + line_peers)

    def rim_copy():
        return pltpu.make_async_remote_copy(
            src_ref=feats_ref.at[pl.ds(rows - reach_rows, reach_rows)],
            dst_ref=wide.at[pl.ds(0, reach_rows)],
            send_sem=rim_send, recv_sem=rim_recv,
            device_id={"tp": jnp.minimum(me + 1, n_tp - 1)}, device_id_type=MESH,
        )

    @pl.when(me < n_tp - 1)
    def _():
        rim_copy().start()

    sec_copies = []
    for c in range(3):
        for d in range(1, n_sec):
            copy = pltpu.make_async_remote_copy(
                src_ref=part_out.at[c], dst_ref=part_in.at[d - 1, c],
                send_sem=sec_send.at[d - 1, c], recv_sem=sec_recv.at[d - 1, c],
                device_id={"sec": sec_peers[d - 1]}, device_id_type=MESH,
            )
            copy.start()
            sec_copies.append(copy)

    @pl.when(me == 0)
    def _():
        wide[pl.ds(0, reach_rows), :] = jnp.zeros((reach_rows, fin), BF16)

    loads[4].wait()
    loads[5].wait()

    @pl.when(me > 0)
    def _():
        rim_copy().wait_recv()

    row = me * rows + lax.broadcasted_iota(jnp.int32, (rows, 1), 0)
    own_clip = clip_at(row)
    summed = None
    for delay in range(taps):
        contrib = dot32(wide[pl.ds(reach_rows - delay * VP, rows), :], conv[delay])
        if delay:
            before = row - delay * VP
            in_clip = (before >= 0) & (clip_at(before) == own_clip)
            summed = summed + jnp.where(in_clip, contrib, 0.0)
        else:
            summed = contrib
    latents[me] = summed.astype(BF16)
    lat_copies = []
    for d in range(1, n_tp):
        copy = pltpu.make_async_remote_copy(
            src_ref=latents.at[me], dst_ref=latents.at[me],
            send_sem=lat_send.at[d - 1], recv_sem=lat_recv.at[d - 1],
            device_id={"tp": tp_peers[d - 1]}, device_id_type=MESH,
        )
        copy.start()
        lat_copies.append(copy)

    def line_copy(src, dst, way, c, target):
        return pltpu.make_async_remote_copy(
            src_ref=src.at[c], dst_ref=dst.at[c],
            send_sem=dp_send.at[way, c], recv_sem=dp_recv.at[way, c],
            device_id={"dp": jnp.clip(target, 0, n_dp - 1)}, device_id_type=MESH,
        )

    def to_right(c):
        return line_copy(right_out, left_in, 0, c, dp + 1)

    def to_left(c):
        return line_copy(left_out, right_in, 1, c, dp - 1)

    for c in range(3):
        sum_here = own_sum[c]
        for d in range(1, n_sec):
            sec_copies[c * (n_sec - 1) + d - 1].wait_recv()
            sum_here = sum_here + part_in[d - 1, c].astype(F32)
        own_sum[c] = sum_here
        if n_dp > 1:
            @pl.when(dp == 0)
            def _():
                right_out[c] = sum_here.astype(BF16)
                to_right(c).start()

            @pl.when(dp == n_dp - 1)
            def _():
                left_out[c] = sum_here.astype(BF16)
                to_left(c).start()

    def pass_right():
        for c in range(3):
            @pl.when(dp > 0)
            def _():
                to_right(c).wait_recv()

            @pl.when((dp > 0) & (dp < n_dp - 1))
            def _():
                right_out[c] = (own_sum[c] + left_in[c].astype(F32)).astype(BF16)
                to_right(c).start()

    def pass_left():
        for c in range(3):
            @pl.when(dp < n_dp - 1)
            def _():
                to_left(c).wait_recv()

            @pl.when((dp > 0) & (dp < n_dp - 1))
            def _():
                left_out[c] = (own_sum[c] + right_in[c].astype(F32)).astype(BF16)
                to_left(c).start()

    @pl.when(2 * dp < n_dp)
    def _():
        pass_right()

    pass_left()

    @pl.when(2 * dp >= n_dp)
    def _():
        pass_right()

    for copy in lat_copies:
        copy.wait_recv()
    latent = latents[...].reshape(total, pd)

    def projected(c):
        full = own_sum[c]
        if n_dp > 1:
            full = full + jnp.where(dp > 0, left_in[c].astype(F32), 0.0)
            full = full + jnp.where(dp < n_dp - 1, right_in[c].astype(F32), 0.0)
        high = full.astype(BF16)
        low = (full - high.astype(F32)).astype(BF16)
        both = dot32(latent, jnp.concatenate([high, low], axis=1))
        return both[:, :HD] + both[:, HD:]

    def normed(value, gain):
        scale = lax.rsqrt(jnp.mean(value * value, axis=-1, keepdims=True) + 1e-06)
        return (value * scale * gain).astype(BF16)

    queries[...] = normed(projected(0), gq_ref[...])
    keys[...] = normed(projected(1), gk_ref[...])
    values[...] = projected(2).astype(BF16)

    key_row = lax.broadcasted_iota(jnp.int32, (1, total), 1)
    key_clip = clip_at(key_row)
    key_place = jnp.zeros_like(key_clip)
    for c in range(clip_count):
        key_place = jnp.where(key_clip == c, place_of[c], key_place)

    def attend(block):
        token = block * rows + lax.broadcasted_iota(jnp.int32, (rows, 1), 0)
        place = jnp.zeros_like(token)
        shift = jnp.zeros_like(token) + place_shift[0] * VP
        for r in range(1, clip_count):
            here = token >= place_start[r] * VP
            place = place + here.astype(jnp.int32)
            shift = jnp.where(here, place_shift[r] * VP, shift)
        picks = jnp.where(token + shift == key_row, 1.0, 0.0).astype(BF16)
        query = dot32(picks, queries[...]).astype(BF16)
        scores = lax.dot_general(
            query, keys[...], (((1,), (1,)), ((), ())), preferred_element_type=F32
        )
        scores = jnp.where(place == key_place, scores, -1e30)
        highest = jnp.max(scores, axis=-1, keepdims=True)
        expo = jnp.exp((scores - highest) * HD ** (-0.5))
        weight = jnp.sum(expo, axis=-1, keepdims=True)
        return (dot32(expo.astype(BF16), values[...]) / weight).astype(BF16)

    out_copies = []
    for d in sorted(range(1, n_tp), key=lambda d: abs(2 * d - n_tp)):
        peer = tp_peers[d - 1]
        mixed[d - 1] = attend(peer)
        copy = pltpu.make_async_remote_copy(
            src_ref=mixed.at[d - 1], dst_ref=out_ref.at[me],
            send_sem=out_send.at[d - 1], recv_sem=out_recv.at[d - 1],
            device_id={"tp": peer}, device_id_type=MESH,
        )
        copy.start()
        out_copies.append(copy)
    out_ref[me] = attend(me)

    for copy in sec_copies + lat_copies:
        copy.wait_send()

    @pl.when(me < n_tp - 1)
    def _():
        rim_copy().wait_send()

    @pl.when(dp < n_dp - 1)
    def _():
        for c in range(3):
            to_right(c).wait_send()

    @pl.when(dp > 0)
    def _():
        for c in range(3):
            to_left(c).wait_send()

    for copy in out_copies:
        copy.wait()


def local(sizes, feats, frame_clip, clip_order, conv_weight, embed_weight, wq, wk, wv, q_gain, k_gain):
    n_sec, n_tp, n_dp = sizes
    feature = feats[0]
    rows, fin = feature.shape
    taps, _, pd = conv_weight.shape
    depth = wq.shape[0]
    total = rows * n_tp
    direct_embed = depth % 128 == 0
    if not direct_embed:
        slot = lax.axis_index("sec") * n_dp + lax.axis_index("dp")
        embed_weight = lax.dynamic_slice_in_dim(embed_weight, slot * depth, depth, 1)
    hbm, vmem, smem = (
        pl.BlockSpec(memory_space=space) for space in (pl.ANY, pltpu.VMEM, pltpu.SMEM)
    )
    dma = pltpu.SemaphoreType.DMA
    sec_links, tp_links = max(1, n_sec - 1), max(1, n_tp - 1)
    pieces = (3, pd, HD)
    out = pl.pallas_call(
        functools.partial(kernel, sizes, direct_embed),
        out_shape=jax.ShapeDtypeStruct((n_tp, rows, HD), BF16),
        in_specs=[smem, smem, hbm, hbm, hbm, hbm, hbm, hbm, vmem, vmem],
        out_specs=vmem,
        scratch_shapes=[
            pltpu.VMEM(((taps - 1) * VP + rows, fin), BF16),
            pltpu.VMEM(conv_weight.shape, BF16),
            pltpu.VMEM((pd, depth), BF16),
            pltpu.VMEM((3, depth, HD), BF16),
            pltpu.VMEM(pieces, BF16),
            pltpu.VMEM((sec_links,) + pieces, BF16),
            pltpu.VMEM(pieces, F32),
            pltpu.VMEM(pieces, BF16),
            pltpu.VMEM(pieces, BF16),
            pltpu.VMEM(pieces, BF16),
            pltpu.VMEM(pieces, BF16),
            pltpu.VMEM((n_tp, rows, pd), BF16),
            pltpu.VMEM((total, HD), BF16),
            pltpu.VMEM((total, HD), BF16),
            pltpu.VMEM((total, HD), BF16),
            pltpu.VMEM((tp_links, rows, HD), BF16),
            dma((6,)),
            dma(()),
            dma(()),
            dma((sec_links, 3)),
            dma((sec_links, 3)),
            dma((2, 3)),
            dma((2, 3)),
            dma((tp_links,)),
            dma((tp_links,)),
            dma((tp_links,)),
            dma((tp_links,)),
        ],
        compiler_params=pltpu.CompilerParams(collective_id=0, has_side_effects=True),
    )(frame_clip, clip_order, feature, conv_weight, embed_weight, wq, wk, wv, q_gain, k_gain)
    return jnp.transpose(out, (1, 0, 2)).reshape(1, rows, n_tp * HD)


def solution(mesh):
    sizes = tuple(mesh.shape[name] for name in ("sec", "tp", "dp"))
    return jax.shard_map(
        functools.partial(local, sizes),
        mesh=mesh,
        in_specs=(
            P(("sec", "dp"), "tp", None),
            P(("sec", "dp"), None),
            P(("sec", "dp"), None),
            P(),
            P(),
            P(("sec", "dp"), "tp"),
            P(("sec", "dp"), "tp"),
            P(("sec", "dp"), "tp"),
            P("tp", None),
            P("tp", None),
        ),
        out_specs=P(("sec", "dp"), "tp", None),
        check_vma=False,
    )
```

```python
import functools
import jax
import jax.numpy as jnp
from jax import lax
from jax.experimental import pallas as pl
from jax.experimental.pallas import tpu as pltpu
from jax.sharding import PartitionSpec as P

HD = 128
VP = 16
MESH = pl.DeviceIdType.MESH
BF16 = jnp.bfloat16
F32 = jnp.float32


def dot32(a, b):
    return jnp.dot(a, b, preferred_element_type=F32)


def dot_t(a, b):
    return lax.dot_general(a, b, (((1,), (1,)), ((), ())), preferred_element_type=F32)


def partner(index, step, count):
    if count & (count - 1):
        return lax.rem(index + step, count)
    peer, weight = 0, 1
    while weight < count:
        bit = lax.rem(lax.div(index, weight), 2)
        peer = peer + weight * (1 - bit if step & weight else bit)
        weight *= 2
    return peer


def kernel(
    sizes, direct_embed,
    frame_ref, order_ref, feats_ref, conv_ref, embed_ref, wq_ref, wk_ref, wv_ref, gq_ref, gk_ref,
    out_ref,
    wide, conv, embed, weights, own_sum, sec_out, sec_in, left_in, left_out, right_in, right_out,
    latents, queries, keys, values, mixed,
    local_sem, rim_send, rim_recv, sec_send, sec_recv, dp_send, dp_recv, lat_send, lat_recv, out_send, out_recv,
):
    n_sec, n_tp, n_dp = sizes
    sec, me, dp = lax.axis_index("sec"), lax.axis_index("tp"), lax.axis_index("dp")
    rows = feats_ref.shape[0]
    taps, pd, fin = conv_ref.shape
    depth = wq_ref.shape[0]
    reach_rows = (taps - 1) * VP
    total = rows * n_tp
    frame_count = frame_ref.shape[1]
    clip_count = order_ref.shape[1]
    sec_peers = [lax.rem(sec + d, n_sec) for d in range(1, n_sec)]
    tp_peers = [partner(me, d, n_tp) for d in range(1, n_tp)]

    barrier = pltpu.get_barrier_semaphore()

    def greet(where):
        pl.semaphore_signal(barrier, inc=1, device_id=where, device_id_type=MESH)

    for peer in sec_peers:
        greet({"sec": peer})
    for peer in tp_peers:
        greet({"tp": peer})

    @pl.when(dp > 0)
    def _():
        greet({"dp": dp - 1})

    @pl.when(dp < n_dp - 1)
    def _():
        greet({"dp": dp + 1})

    if direct_embed:
        begin = pl.multiple_of((sec * n_dp + dp) * depth, 128)
        embed_from = embed_ref.at[:, pl.ds(begin, depth)]
    else:
        embed_from = embed_ref
    loads = [
        pltpu.make_async_copy(embed_from, embed, local_sem.at[0]),
        pltpu.make_async_copy(wq_ref, weights.at[0], local_sem.at[1]),
        pltpu.make_async_copy(wk_ref, weights.at[1], local_sem.at[2]),
        pltpu.make_async_copy(wv_ref, weights.at[2], local_sem.at[3]),
        pltpu.make_async_copy(feats_ref, wide.at[pl.ds(reach_rows, rows)], local_sem.at[4]),
        pltpu.make_async_copy(conv_ref, conv, local_sem.at[5]),
    ]
    for load in loads:
        load.start()

    first = [jnp.int32(0) for _ in range(clip_count)]
    for f in range(frame_count):
        clip = frame_ref[0, f]
        for c in range(1, clip_count):
            first[c] = first[c] + (clip < c).astype(jnp.int32)
    lengths = [
        (first[c + 1] if c + 1 < clip_count else jnp.int32(frame_count)) - first[c]
        for c in range(clip_count)
    ]
    place_start, place_shift, place_of = [], [], [jnp.int32(0) for _ in range(clip_count)]
    running = jnp.int32(0)
    for r in range(clip_count):
        clip = order_ref[0, r]
        length, start = jnp.int32(0), jnp.int32(0)
        for c in range(clip_count):
            here = clip == c
            length = jnp.where(here, lengths[c], length)
            start = jnp.where(here, first[c], start)
            place_of[c] = jnp.where(here, r, place_of[c])
        place_start.append(running)
        place_shift.append(start - running)
        running = running + length

    def clip_at(row):
        clip = jnp.zeros_like(row)
        for c in range(1, clip_count):
            clip = clip + (row >= first[c] * VP).astype(jnp.int32)
        return clip

    line_peers = (dp > 0).astype(jnp.int32) + (dp < n_dp - 1).astype(jnp.int32)
    pl.semaphore_wait(barrier, (n_sec - 1) + (n_tp - 1) + line_peers)

    def rim_copy():
        return pltpu.make_async_remote_copy(
            src_ref=feats_ref.at[pl.ds(rows - reach_rows, reach_rows)],
            dst_ref=wide.at[pl.ds(0, reach_rows)],
            send_sem=rim_send, recv_sem=rim_recv,
            device_id={"tp": jnp.minimum(me + 1, n_tp - 1)}, device_id_type=MESH,
        )

    @pl.when(me < n_tp - 1)
    def _():
        rim_copy().start()

    @pl.when(me == 0)
    def _():
        wide[pl.ds(0, reach_rows), :] = jnp.zeros((reach_rows, fin), BF16)

    def sec_copy(half, c, d):
        return pltpu.make_async_remote_copy(
            src_ref=sec_out.at[half, c], dst_ref=sec_in.at[d - 1, half, c],
            send_sem=sec_send.at[d - 1, half, c], recv_sem=sec_recv.at[d - 1, half, c],
            device_id={"sec": sec_peers[d - 1]}, device_id_type=MESH,
        )

    def send_sec(half, c):
        for d in range(1, n_sec):
            sec_copy(half, c, d).start()

    def add_sec(half, c):
        sum_here = own_sum[half, c]
        for d in range(1, n_sec):
            sec_copy(half, c, d).wait_recv()
            sum_here = sum_here + sec_in[d - 1, half, c].astype(F32)
        return sum_here

    def line_copy(src, dst, way, half, c, target):
        return pltpu.make_async_remote_copy(
            src_ref=src.at[half, c], dst_ref=dst.at[half, c],
            send_sem=dp_send.at[way, half, c], recv_sem=dp_recv.at[way, half, c],
            device_id={"dp": jnp.clip(target, 0, n_dp - 1)}, device_id_type=MESH,
        )

    def to_right(half, c):
        return line_copy(right_out, left_in, 0, half, c, dp + 1)

    def to_left(half, c):
        return line_copy(left_out, right_in, 1, half, c, dp - 1)

    def begin_line(half, c, value):
        if n_dp > 1:
            @pl.when(dp == 0)
            def _():
                right_out[half, c] = value
                to_right(half, c).start()

            @pl.when(dp == n_dp - 1)
            def _():
                left_out[half, c] = value
                to_left(half, c).start()

    def pass_right(half):
        for c in range(3):
            @pl.when(dp > 0)
            def _():
                to_right(half, c).wait_recv()

            @pl.when((dp > 0) & (dp < n_dp - 1))
            def _():
                right_out[half, c] = (own_sum[half, c] + left_in[half, c].astype(F32)).astype(BF16)
                to_right(half, c).start()

    def pass_left(half):
        for c in range(3):
            @pl.when(dp < n_dp - 1)
            def _():
                to_left(half, c).wait_recv()

            @pl.when((dp > 0) & (dp < n_dp - 1))
            def _():
                left_out[half, c] = (own_sum[half, c] + right_in[half, c].astype(F32)).astype(BF16)
                to_left(half, c).start()

    def line_sum(half, c):
        full = own_sum[half, c]
        if n_dp > 1:
            full = full + jnp.where(dp > 0, left_in[half, c].astype(F32), 0.0)
            full = full + jnp.where(dp < n_dp - 1, right_in[half, c].astype(F32), 0.0)
        return full

    half_rows = pd // 2
    loads[0].wait()
    for c in range(3):
        loads[1 + c].wait()
        partial = dot32(embed[...], weights[c])
        for half in range(2):
            piece = partial[half * half_rows : (half + 1) * half_rows]
            own_sum[half, c] = piece
            if half == 0:
                sec_out[0, c] = piece.astype(BF16)
                send_sec(0, c)
            else:
                begin_line(1, c, piece.astype(BF16))

    loads[4].wait()
    loads[5].wait()

    @pl.when(me > 0)
    def _():
        rim_copy().wait_recv()

    row = me * rows + lax.broadcasted_iota(jnp.int32, (rows, 1), 0)
    own_clip = clip_at(row)
    summed = None
    for delay in range(taps):
        contrib = dot_t(wide[pl.ds(reach_rows - delay * VP, rows), :], conv[delay])
        if delay:
            before = row - delay * VP
            in_clip = (before >= 0) & (clip_at(before) == own_clip)
            summed = summed + jnp.where(in_clip, contrib, 0.0)
        else:
            summed = contrib
    latents[me] = summed.astype(BF16)
    lat_copies = []
    for d in range(n_tp - 1, 0, -1):
        copy = pltpu.make_async_remote_copy(
            src_ref=latents.at[me], dst_ref=latents.at[me],
            send_sem=lat_send.at[d - 1], recv_sem=lat_recv.at[d - 1],
            device_id={"tp": tp_peers[d - 1]}, device_id_type=MESH,
        )
        copy.start()
        lat_copies.append(copy)

    for c in range(3):
        sum_here = add_sec(0, c)
        own_sum[0, c] = sum_here
        begin_line(0, c, sum_here.astype(BF16))

    @pl.when(2 * dp < n_dp)
    def _():
        pass_right(1)
        pass_right(0)
        pass_left(1)

    @pl.when(2 * dp >= n_dp)
    def _():
        pass_left(1)
        pass_left(0)
        pass_right(1)

    for c in range(3):
        sum_here = line_sum(1, c)
        own_sum[1, c] = sum_here
        sec_out[1, c] = sum_here.astype(BF16)
        send_sec(1, c)

    @pl.when(2 * dp < n_dp)
    def _():
        pass_left(0)

    @pl.when(2 * dp >= n_dp)
    def _():
        pass_right(0)

    for copy in lat_copies:
        copy.wait_recv()
    latent = latents[...].reshape(total, pd)

    def projected(c):
        full = jnp.concatenate([line_sum(0, c), add_sec(1, c)], axis=0)
        high = full.astype(BF16)
        low = (full - high.astype(F32)).astype(BF16)
        both = dot32(latent, jnp.concatenate([high, low], axis=1))
        return both[:, :HD] + both[:, HD:]

    def normed(value, gain):
        scale = lax.rsqrt(jnp.mean(value * value, axis=-1, keepdims=True) + 1e-06)
        return (value * scale * gain).astype(BF16)

    queries[...] = normed(projected(0), gq_ref[...])
    keys[...] = normed(projected(1), gk_ref[...])
    values[...] = projected(2).astype(BF16)

    key_row = lax.broadcasted_iota(jnp.int32, (1, total), 1)
    key_clip = clip_at(key_row)
    key_place = jnp.zeros_like(key_clip)
    for c in range(clip_count):
        key_place = jnp.where(key_clip == c, place_of[c], key_place)

    def attend(block):
        token = block * rows + lax.broadcasted_iota(jnp.int32, (rows, 1), 0)
        place = jnp.zeros_like(token)
        shift = jnp.zeros_like(token) + place_shift[0] * VP
        for r in range(1, clip_count):
            here = token >= place_start[r] * VP
            place = place + here.astype(jnp.int32)
            shift = jnp.where(here, place_shift[r] * VP, shift)
        picks = jnp.where(token + shift == key_row, 1.0, 0.0).astype(BF16)
        query = dot32(picks, queries[...]).astype(BF16)
        scores = dot_t(query, keys[...])
        scores = jnp.where(place == key_place, scores, -1e30)
        highest = jnp.max(scores, axis=-1, keepdims=True)
        expo = jnp.exp((scores - highest) * HD ** (-0.5))
        weight = jnp.sum(expo, axis=-1, keepdims=True)
        return (dot32(expo.astype(BF16), values[...]) / weight).astype(BF16)

    def columns(head):
        return pl.ds(pl.multiple_of(head * HD, HD), HD)

    out_copies = []
    for d in range(n_tp - 1, 0, -1):
        peer = tp_peers[d - 1]
        mixed[d - 1] = attend(peer)
        copy = pltpu.make_async_remote_copy(
            src_ref=mixed.at[d - 1], dst_ref=out_ref.at[:, columns(me)],
            send_sem=out_send.at[d - 1], recv_sem=out_recv.at[d - 1],
            device_id={"tp": peer}, device_id_type=MESH,
        )
        copy.start()
        out_copies.append(copy)
    out_ref[:, columns(me)] = attend(me)

    for copy in lat_copies:
        copy.wait_send()
    for half in range(2):
        for c in range(3):
            for d in range(1, n_sec):
                sec_copy(half, c, d).wait_send()

    @pl.when(me < n_tp - 1)
    def _():
        rim_copy().wait_send()

    @pl.when(dp < n_dp - 1)
    def _():
        for half in range(2):
            for c in range(3):
                to_right(half, c).wait_send()

    @pl.when(dp > 0)
    def _():
        for half in range(2):
            for c in range(3):
                to_left(half, c).wait_send()

    for copy in out_copies:
        copy.wait()


def local(sizes, feats, frame_clip, clip_order, conv_weight, embed_weight, wq, wk, wv, q_gain, k_gain):
    n_sec, n_tp, n_dp = sizes
    feature = feats[0]
    rows, fin = feature.shape
    conv_weight = jnp.swapaxes(conv_weight, 1, 2)
    taps, pd, _ = conv_weight.shape
    depth = wq.shape[0]
    total = rows * n_tp
    direct_embed = depth % 128 == 0
    if not direct_embed:
        slot = lax.axis_index("sec") * n_dp + lax.axis_index("dp")
        embed_weight = lax.dynamic_slice_in_dim(embed_weight, slot * depth, depth, 1)
    hbm, vmem, smem = (
        pl.BlockSpec(memory_space=space) for space in (pl.ANY, pltpu.VMEM, pltpu.SMEM)
    )
    dma = pltpu.SemaphoreType.DMA
    sec_links, tp_links = max(1, n_sec - 1), max(1, n_tp - 1)
    pieces = (2, 3, pd // 2, HD)
    out = pl.pallas_call(
        functools.partial(kernel, sizes, direct_embed),
        out_shape=jax.ShapeDtypeStruct((rows, n_tp * HD), BF16),
        in_specs=[smem, smem, hbm, hbm, hbm, hbm, hbm, hbm, vmem, vmem],
        out_specs=vmem,
        scratch_shapes=[
            pltpu.VMEM(((taps - 1) * VP + rows, fin), BF16),
            pltpu.VMEM(conv_weight.shape, BF16),
            pltpu.VMEM((pd, depth), BF16),
            pltpu.VMEM((3, depth, HD), BF16),
            pltpu.VMEM(pieces, F32),
            pltpu.VMEM(pieces, BF16),
            pltpu.VMEM((sec_links,) + pieces, BF16),
            pltpu.VMEM(pieces, BF16),
            pltpu.VMEM(pieces, BF16),
            pltpu.VMEM(pieces, BF16),
            pltpu.VMEM(pieces, BF16),
            pltpu.VMEM((n_tp, rows, pd), BF16),
            pltpu.VMEM((total, HD), BF16),
            pltpu.VMEM((total, HD), BF16),
            pltpu.VMEM((total, HD), BF16),
            pltpu.VMEM((tp_links, rows, HD), BF16),
            dma((6,)),
            dma(()),
            dma(()),
            dma((sec_links, 2, 3)),
            dma((sec_links, 2, 3)),
            dma((2, 2, 3)),
            dma((2, 2, 3)),
            dma((tp_links,)),
            dma((tp_links,)),
            dma((tp_links,)),
            dma((tp_links,)),
        ],
        compiler_params=pltpu.CompilerParams(collective_id=0, has_side_effects=True),
    )(frame_clip, clip_order, feature, conv_weight, embed_weight, wq, wk, wv, q_gain, k_gain)
    return out[None]


def solution(mesh):
    sizes = tuple(mesh.shape[name] for name in ("sec", "tp", "dp"))
    return jax.shard_map(
        functools.partial(local, sizes),
        mesh=mesh,
        in_specs=(
            P(("sec", "dp"), "tp", None),
            P(("sec", "dp"), None),
            P(("sec", "dp"), None),
            P(),
            P(),
            P(("sec", "dp"), "tp"),
            P(("sec", "dp"), "tp"),
            P(("sec", "dp"), "tp"),
            P("tp", None),
            P("tp", None),
        ),
        out_specs=P(("sec", "dp"), "tp", None),
        check_vma=False,
    )
```

```python
import functools
import jax
import jax.numpy as jnp
from jax import lax
from jax.experimental import pallas as pl
from jax.experimental.pallas import tpu as pltpu
from jax.sharding import PartitionSpec as P

HD = 128
VP = 16
MESH = pl.DeviceIdType.MESH
BF16 = jnp.bfloat16
F32 = jnp.float32


def dot32(a, b):
    return jnp.dot(a, b, preferred_element_type=F32)


def dot_t(a, b):
    return lax.dot_general(a, b, (((1,), (1,)), ((), ())), preferred_element_type=F32)


def partner(index, step, count):
    if count & (count - 1):
        return lax.rem(index + step, count)
    peer, weight = 0, 1
    while weight < count:
        bit = lax.rem(lax.div(index, weight), 2)
        peer = peer + weight * (1 - bit if step & weight else bit)
        weight *= 2
    return peer


def kernel(
    sizes, direct_embed,
    frame_ref, order_ref, feats_ref, conv_ref, embed_ref, wq_ref, wk_ref, wv_ref, gq_ref, gk_ref,
    out_ref,
    wide, conv, embed, weights, own_sum, sec_out, sec_in, left_in, left_out, right_in, right_out,
    latents, queries, keys, values, mixed,
    local_sem, rim_send, rim_recv, sec_send, sec_recv, dp_send, dp_recv, lat_send, lat_recv, out_send, out_recv,
):
    n_sec, n_tp, n_dp = sizes
    sec, me, dp = lax.axis_index("sec"), lax.axis_index("tp"), lax.axis_index("dp")
    rows = feats_ref.shape[0]
    taps, pd, fin = conv_ref.shape
    depth = wq_ref.shape[0]
    reach_rows = (taps - 1) * VP
    total = rows * n_tp
    frame_count = frame_ref.shape[1]
    clip_count = order_ref.shape[1]
    sec_peers = [lax.rem(sec + d, n_sec) for d in range(1, n_sec)]
    tp_peers = [partner(me, d, n_tp) for d in range(1, n_tp)]

    barrier = pltpu.get_barrier_semaphore()

    def greet(where):
        pl.semaphore_signal(barrier, inc=1, device_id=where, device_id_type=MESH)

    for peer in sec_peers:
        greet({"sec": peer})
    for peer in tp_peers:
        greet({"tp": peer})

    @pl.when(dp > 0)
    def _():
        greet({"dp": dp - 1})

    @pl.when(dp < n_dp - 1)
    def _():
        greet({"dp": dp + 1})

    if direct_embed:
        begin = pl.multiple_of((sec * n_dp + dp) * depth, 128)
        embed_from = embed_ref.at[:, pl.ds(begin, depth)]
    else:
        embed_from = embed_ref
    loads = [
        pltpu.make_async_copy(embed_from, embed, local_sem.at[0]),
        pltpu.make_async_copy(wq_ref, weights.at[0], local_sem.at[1]),
        pltpu.make_async_copy(wk_ref, weights.at[1], local_sem.at[2]),
        pltpu.make_async_copy(wv_ref, weights.at[2], local_sem.at[3]),
        pltpu.make_async_copy(feats_ref, wide.at[pl.ds(reach_rows, rows)], local_sem.at[4]),
        pltpu.make_async_copy(conv_ref, conv, local_sem.at[5]),
    ]
    for load in loads:
        load.start()

    first = [jnp.int32(0) for _ in range(clip_count)]
    for f in range(frame_count):
        clip = frame_ref[0, f]
        for c in range(1, clip_count):
            first[c] = first[c] + (clip < c).astype(jnp.int32)
    lengths = [
        (first[c + 1] if c + 1 < clip_count else jnp.int32(frame_count)) - first[c]
        for c in range(clip_count)
    ]
    place_start, place_shift, place_of = [], [], [jnp.int32(0) for _ in range(clip_count)]
    running = jnp.int32(0)
    for r in range(clip_count):
        clip = order_ref[0, r]
        length, start = jnp.int32(0), jnp.int32(0)
        for c in range(clip_count):
            here = clip == c
            length = jnp.where(here, lengths[c], length)
            start = jnp.where(here, first[c], start)
            place_of[c] = jnp.where(here, r, place_of[c])
        place_start.append(running)
        place_shift.append(start - running)
        running = running + length

    def clip_at(row):
        clip = jnp.zeros_like(row)
        for c in range(1, clip_count):
            clip = clip + (row >= first[c] * VP).astype(jnp.int32)
        return clip

    line_peers = (dp > 0).astype(jnp.int32) + (dp < n_dp - 1).astype(jnp.int32)
    pl.semaphore_wait(barrier, (n_sec - 1) + (n_tp - 1) + line_peers)

    def rim_copy():
        return pltpu.make_async_remote_copy(
            src_ref=feats_ref.at[pl.ds(rows - reach_rows, reach_rows)],
            dst_ref=wide.at[pl.ds(0, reach_rows)],
            send_sem=rim_send, recv_sem=rim_recv,
            device_id={"tp": jnp.minimum(me + 1, n_tp - 1)}, device_id_type=MESH,
        )

    @pl.when(me < n_tp - 1)
    def _():
        rim_copy().start()

    @pl.when(me == 0)
    def _():
        wide[pl.ds(0, reach_rows), :] = jnp.zeros((reach_rows, fin), BF16)

    def sec_copy(half, c, d):
        return pltpu.make_async_remote_copy(
            src_ref=sec_out.at[half, c], dst_ref=sec_in.at[d - 1, half, c],
            send_sem=sec_send.at[d - 1, half, c], recv_sem=sec_recv.at[d - 1, half, c],
            device_id={"sec": sec_peers[d - 1]}, device_id_type=MESH,
        )

    def send_sec(half, c):
        for d in range(1, n_sec):
            sec_copy(half, c, d).start()

    def add_sec(half, c):
        sum_here = own_sum[half, c]
        for d in range(1, n_sec):
            sec_copy(half, c, d).wait_recv()
            sum_here = sum_here + sec_in[d - 1, half, c].astype(F32)
        return sum_here

    def line_copy(src, dst, way, half, c, target):
        return pltpu.make_async_remote_copy(
            src_ref=src.at[half, c], dst_ref=dst.at[half, c],
            send_sem=dp_send.at[way, half, c], recv_sem=dp_recv.at[way, half, c],
            device_id={"dp": jnp.clip(target, 0, n_dp - 1)}, device_id_type=MESH,
        )

    def to_right(half, c):
        return line_copy(right_out, left_in, 0, half, c, dp + 1)

    def to_left(half, c):
        return line_copy(left_out, right_in, 1, half, c, dp - 1)

    def begin_line(half, c, value):
        if n_dp > 1:
            @pl.when(dp == 0)
            def _():
                right_out[half, c] = value
                to_right(half, c).start()

            @pl.when(dp == n_dp - 1)
            def _():
                left_out[half, c] = value
                to_left(half, c).start()

    def pass_right(half, c):
        @pl.when(dp > 0)
        def _():
            to_right(half, c).wait_recv()

        @pl.when((dp > 0) & (dp < n_dp - 1))
        def _():
            right_out[half, c] = (own_sum[half, c] + left_in[half, c].astype(F32)).astype(BF16)
            to_right(half, c).start()

    def pass_left(half, c):
        @pl.when(dp < n_dp - 1)
        def _():
            to_left(half, c).wait_recv()

        @pl.when((dp > 0) & (dp < n_dp - 1))
        def _():
            left_out[half, c] = (own_sum[half, c] + right_in[half, c].astype(F32)).astype(BF16)
            to_left(half, c).start()

    def line_sum(half, c):
        full = own_sum[half, c]
        if n_dp > 1:
            full = full + jnp.where(dp > 0, left_in[half, c].astype(F32), 0.0)
            full = full + jnp.where(dp < n_dp - 1, right_in[half, c].astype(F32), 0.0)
        return full

    half_rows = pd // 2
    loads[0].wait()
    for c in range(3):
        loads[1 + c].wait()
        partial = dot32(embed[...], weights[c])
        for half in range(2):
            piece = partial[half * half_rows : (half + 1) * half_rows]
            own_sum[half, c] = piece
            if half == 0:
                sec_out[0, c] = piece.astype(BF16)
                send_sec(0, c)
            else:
                begin_line(1, c, piece.astype(BF16))

    loads[4].wait()
    loads[5].wait()

    @pl.when(me > 0)
    def _():
        rim_copy().wait_recv()

    row = me * rows + lax.broadcasted_iota(jnp.int32, (rows, 1), 0)
    own_clip = clip_at(row)
    summed = None
    for delay in range(taps):
        contrib = dot_t(wide[pl.ds(reach_rows - delay * VP, rows), :], conv[delay])
        if delay:
            before = row - delay * VP
            in_clip = (before >= 0) & (clip_at(before) == own_clip)
            summed = summed + jnp.where(in_clip, contrib, 0.0)
        else:
            summed = contrib
    latents[me] = summed.astype(BF16)
    lat_copies = []
    for d in range(n_tp - 1, 0, -1):
        copy = pltpu.make_async_remote_copy(
            src_ref=latents.at[me], dst_ref=latents.at[me],
            send_sem=lat_send.at[d - 1], recv_sem=lat_recv.at[d - 1],
            device_id={"tp": tp_peers[d - 1]}, device_id_type=MESH,
        )
        copy.start()
        lat_copies.append(copy)

    for c in range(3):
        sum_here = add_sec(0, c)
        own_sum[0, c] = sum_here
        begin_line(0, c, sum_here.astype(BF16))

        @pl.when(2 * dp < n_dp)
        def _():
            pass_right(1, c)

        @pl.when(2 * dp >= n_dp)
        def _():
            pass_left(1, c)

    for c in range(3):
        @pl.when(2 * dp < n_dp)
        def _():
            pass_left(1, c)

        @pl.when(2 * dp >= n_dp)
        def _():
            pass_right(1, c)

        sum_here = line_sum(1, c)
        own_sum[1, c] = sum_here
        sec_out[1, c] = sum_here.astype(BF16)
        send_sec(1, c)

        @pl.when(2 * dp < n_dp)
        def _():
            pass_right(0, c)

        @pl.when(2 * dp >= n_dp)
        def _():
            pass_left(0, c)

    for c in range(3):
        @pl.when(2 * dp < n_dp)
        def _():
            pass_left(0, c)

        @pl.when(2 * dp >= n_dp)
        def _():
            pass_right(0, c)

    for copy in lat_copies:
        copy.wait_recv()
    latent = latents[...].reshape(total, pd)

    def projected(c):
        full = jnp.concatenate([line_sum(0, c), add_sec(1, c)], axis=0)
        high = full.astype(BF16)
        low = (full - high.astype(F32)).astype(BF16)
        both = dot32(latent, jnp.concatenate([high, low], axis=1))
        return both[:, :HD] + both[:, HD:]

    def normed(value, gain):
        scale = lax.rsqrt(jnp.mean(value * value, axis=-1, keepdims=True) + 1e-06)
        return (value * scale * gain).astype(BF16)

    queries[...] = normed(projected(0), gq_ref[...])
    keys[...] = normed(projected(1), gk_ref[...])
    values[...] = projected(2).astype(BF16)

    key_row = lax.broadcasted_iota(jnp.int32, (1, total), 1)
    key_clip = clip_at(key_row)
    key_place = jnp.zeros_like(key_clip)
    for c in range(clip_count):
        key_place = jnp.where(key_clip == c, place_of[c], key_place)

    def attend(block):
        token = block * rows + lax.broadcasted_iota(jnp.int32, (rows, 1), 0)
        place = jnp.zeros_like(token)
        shift = jnp.zeros_like(token) + place_shift[0] * VP
        for r in range(1, clip_count):
            here = token >= place_start[r] * VP
            place = place + here.astype(jnp.int32)
            shift = jnp.where(here, place_shift[r] * VP, shift)
        picks = jnp.where(token + shift == key_row, 1.0, 0.0).astype(BF16)
        query = dot32(picks, queries[...]).astype(BF16)
        scores = dot_t(query, keys[...])
        scores = jnp.where(place == key_place, scores, -1e30)
        highest = jnp.max(scores, axis=-1, keepdims=True)
        expo = jnp.exp((scores - highest) * HD ** (-0.5))
        weight = jnp.sum(expo, axis=-1, keepdims=True)
        return (dot32(expo.astype(BF16), values[...]) / weight).astype(BF16)

    def columns(head):
        return pl.ds(pl.multiple_of(head * HD, HD), HD)

    out_copies = []
    for d in range(n_tp - 1, 0, -1):
        peer = tp_peers[d - 1]
        mixed[d - 1] = attend(peer)
        copy = pltpu.make_async_remote_copy(
            src_ref=mixed.at[d - 1], dst_ref=out_ref.at[:, columns(me)],
            send_sem=out_send.at[d - 1], recv_sem=out_recv.at[d - 1],
            device_id={"tp": peer}, device_id_type=MESH,
        )
        copy.start()
        out_copies.append(copy)
    out_ref[:, columns(me)] = attend(me)

    for copy in lat_copies:
        copy.wait_send()
    for half in range(2):
        for c in range(3):
            for d in range(1, n_sec):
                sec_copy(half, c, d).wait_send()

    @pl.when(me < n_tp - 1)
    def _():
        rim_copy().wait_send()

    @pl.when(dp < n_dp - 1)
    def _():
        for half in range(2):
            for c in range(3):
                to_right(half, c).wait_send()

    @pl.when(dp > 0)
    def _():
        for half in range(2):
            for c in range(3):
                to_left(half, c).wait_send()

    for copy in out_copies:
        copy.wait()


def local(sizes, feats, frame_clip, clip_order, conv_weight, embed_weight, wq, wk, wv, q_gain, k_gain):
    n_sec, n_tp, n_dp = sizes
    feature = feats[0]
    rows, fin = feature.shape
    conv_weight = jnp.swapaxes(conv_weight, 1, 2)
    taps, pd, _ = conv_weight.shape
    depth = wq.shape[0]
    total = rows * n_tp
    direct_embed = depth % 128 == 0
    if not direct_embed:
        slot = lax.axis_index("sec") * n_dp + lax.axis_index("dp")
        embed_weight = lax.dynamic_slice_in_dim(embed_weight, slot * depth, depth, 1)
    hbm, vmem, smem = (
        pl.BlockSpec(memory_space=space) for space in (pl.ANY, pltpu.VMEM, pltpu.SMEM)
    )
    dma = pltpu.SemaphoreType.DMA
    sec_links, tp_links = max(1, n_sec - 1), max(1, n_tp - 1)
    pieces = (2, 3, pd // 2, HD)
    out = pl.pallas_call(
        functools.partial(kernel, sizes, direct_embed),
        out_shape=pltpu.VMEM((rows, n_tp * HD), BF16),
        in_specs=[smem, smem, hbm, hbm, hbm, hbm, hbm, hbm, vmem, vmem],
        out_specs=vmem,
        scratch_shapes=[
            pltpu.VMEM(((taps - 1) * VP + rows, fin), BF16),
            pltpu.VMEM(conv_weight.shape, BF16),
            pltpu.VMEM((pd, depth), BF16),
            pltpu.VMEM((3, depth, HD), BF16),
            pltpu.VMEM(pieces, F32),
            pltpu.VMEM(pieces, BF16),
            pltpu.VMEM((sec_links,) + pieces, BF16),
            pltpu.VMEM(pieces, BF16),
            pltpu.VMEM(pieces, BF16),
            pltpu.VMEM(pieces, BF16),
            pltpu.VMEM(pieces, BF16),
            pltpu.VMEM((n_tp, rows, pd), BF16),
            pltpu.VMEM((total, HD), BF16),
            pltpu.VMEM((total, HD), BF16),
            pltpu.VMEM((total, HD), BF16),
            pltpu.VMEM((tp_links, rows, HD), BF16),
            dma((6,)),
            dma(()),
            dma(()),
            dma((sec_links, 2, 3)),
            dma((sec_links, 2, 3)),
            dma((2, 2, 3)),
            dma((2, 2, 3)),
            dma((tp_links,)),
            dma((tp_links,)),
            dma((tp_links,)),
            dma((tp_links,)),
        ],
        compiler_params=pltpu.CompilerParams(collective_id=0, has_side_effects=True),
    )(frame_clip, clip_order, feature, conv_weight, embed_weight, wq, wk, wv, q_gain, k_gain)
    return out[None]


def solution(mesh):
    sizes = tuple(mesh.shape[name] for name in ("sec", "tp", "dp"))
    return jax.shard_map(
        functools.partial(local, sizes),
        mesh=mesh,
        in_specs=(
            P(("sec", "dp"), "tp", None),
            P(("sec", "dp"), None),
            P(("sec", "dp"), None),
            P(),
            P(),
            P(("sec", "dp"), "tp"),
            P(("sec", "dp"), "tp"),
            P(("sec", "dp"), "tp"),
            P("tp", None),
            P("tp", None),
        ),
        out_specs=P(("sec", "dp"), "tp", None),
        check_vma=False,
    )
```

```python
import functools
import jax
import jax.numpy as jnp
from jax import lax
from jax.experimental import pallas as pl
from jax.experimental.pallas import tpu as pltpu
from jax.sharding import PartitionSpec as P

HD = 128
VP = 16
MESH = pl.DeviceIdType.MESH
BF16 = jnp.bfloat16
F32 = jnp.float32


def dot32(a, b):
    return jnp.dot(a, b, preferred_element_type=F32)


def dot_t(a, b):
    return lax.dot_general(a, b, (((1,), (1,)), ((), ())), preferred_element_type=F32)


def partner(index, step, count):
    if count & (count - 1):
        return lax.rem(index + step, count)
    peer, weight = 0, 1
    while weight < count:
        bit = lax.rem(lax.div(index, weight), 2)
        peer = peer + weight * (1 - bit if step & weight else bit)
        weight *= 2
    return peer


def kernel(
    sizes, direct_embed,
    frame_from, order_from, feats_ref, conv_ref, embed_ref, wq_ref, wk_ref, wv_ref, gq_from, gk_from,
    out_ref,
    wide, conv, embed, weights, own_sum, sec_out, sec_in, left_in, left_out, right_in, right_out,
    latents, packed, queries, keys, values, mixed, frame_ref, order_ref, gq_ref, gk_ref,
    local_sem, rim_send, rim_recv, sec_send, sec_recv, dp_send, dp_recv, lat_send, lat_recv, out_send, out_recv,
):
    n_sec, n_tp, n_dp = sizes
    sec, me, dp = lax.axis_index("sec"), lax.axis_index("tp"), lax.axis_index("dp")
    rows = feats_ref.shape[0]
    taps, pd, fin = conv_ref.shape
    depth = wq_ref.shape[0]
    reach_rows = (taps - 1) * VP
    total = rows * n_tp
    frame_count = frame_ref.shape[1]
    clip_count = order_ref.shape[1]
    sec_peers = [lax.rem(sec + d, n_sec) for d in range(1, n_sec)]
    tp_peers = [partner(me, d, n_tp) for d in range(1, n_tp)]

    barrier = pltpu.get_barrier_semaphore()

    def greet(where):
        pl.semaphore_signal(barrier, inc=1, device_id=where, device_id_type=MESH)

    for peer in sec_peers:
        greet({"sec": peer})
    for peer in tp_peers:
        greet({"tp": peer})

    @pl.when(dp > 0)
    def _():
        greet({"dp": dp - 1})

    @pl.when(dp < n_dp - 1)
    def _():
        greet({"dp": dp + 1})

    if direct_embed:
        begin = pl.multiple_of((sec * n_dp + dp) * depth, 128)
        embed_from = embed_ref.at[:, pl.ds(begin, depth)]
    else:
        embed_from = embed_ref
    loads = [
        pltpu.make_async_copy(embed_from, embed, local_sem.at[0]),
        pltpu.make_async_copy(wq_ref, weights.at[0], local_sem.at[1]),
        pltpu.make_async_copy(wk_ref, weights.at[1], local_sem.at[2]),
        pltpu.make_async_copy(wv_ref, weights.at[2], local_sem.at[3]),
        pltpu.make_async_copy(feats_ref, wide.at[pl.ds(reach_rows, rows)], local_sem.at[4]),
        pltpu.make_async_copy(conv_ref, conv, local_sem.at[5]),
        pltpu.make_async_copy(frame_from, frame_ref, local_sem.at[6]),
        pltpu.make_async_copy(order_from, order_ref, local_sem.at[7]),
        pltpu.make_async_copy(gq_from, gq_ref, local_sem.at[8]),
        pltpu.make_async_copy(gk_from, gk_ref, local_sem.at[9]),
    ]
    for load in loads:
        load.start()

    line_peers = (dp > 0).astype(jnp.int32) + (dp < n_dp - 1).astype(jnp.int32)
    pl.semaphore_wait(barrier, (n_sec - 1) + (n_tp - 1) + line_peers)

    def rim_copy():
        return pltpu.make_async_remote_copy(
            src_ref=feats_ref.at[pl.ds(rows - reach_rows, reach_rows)],
            dst_ref=wide.at[pl.ds(0, reach_rows)],
            send_sem=rim_send, recv_sem=rim_recv,
            device_id={"tp": jnp.minimum(me + 1, n_tp - 1)}, device_id_type=MESH,
        )

    @pl.when(me < n_tp - 1)
    def _():
        rim_copy().start()

    @pl.when(me == 0)
    def _():
        wide[pl.ds(0, reach_rows), :] = jnp.zeros((reach_rows, fin), BF16)

    def sec_copy(half, c, d):
        return pltpu.make_async_remote_copy(
            src_ref=sec_out.at[half, c], dst_ref=sec_in.at[d - 1, half, c],
            send_sem=sec_send.at[d - 1, half, c], recv_sem=sec_recv.at[d - 1, half, c],
            device_id={"sec": sec_peers[d - 1]}, device_id_type=MESH,
        )

    def send_sec(half, c):
        for d in range(1, n_sec):
            sec_copy(half, c, d).start()

    def add_sec(half, c):
        sum_here = own_sum[half, c]
        for d in range(1, n_sec):
            sec_copy(half, c, d).wait_recv()
            sum_here = sum_here + sec_in[d - 1, half, c].astype(F32)
        return sum_here

    def line_copy(src, dst, way, half, c, target):
        return pltpu.make_async_remote_copy(
            src_ref=src.at[half, c], dst_ref=dst.at[half, c],
            send_sem=dp_send.at[way, half, c], recv_sem=dp_recv.at[way, half, c],
            device_id={"dp": jnp.clip(target, 0, n_dp - 1)}, device_id_type=MESH,
        )

    def to_right(half, c):
        return line_copy(right_out, left_in, 0, half, c, dp + 1)

    def to_left(half, c):
        return line_copy(left_out, right_in, 1, half, c, dp - 1)

    def begin_line(half, c, value):
        if n_dp > 1:
            @pl.when(dp == 0)
            def _():
                right_out[half, c] = value
                to_right(half, c).start()

            @pl.when(dp == n_dp - 1)
            def _():
                left_out[half, c] = value
                to_left(half, c).start()

    def pass_right(half, c):
        @pl.when(dp > 0)
        def _():
            to_right(half, c).wait_recv()

        @pl.when((dp > 0) & (dp < n_dp - 1))
        def _():
            right_out[half, c] = (own_sum[half, c] + left_in[half, c].astype(F32)).astype(BF16)
            to_right(half, c).start()

    def pass_left(half, c):
        @pl.when(dp < n_dp - 1)
        def _():
            to_left(half, c).wait_recv()

        @pl.when((dp > 0) & (dp < n_dp - 1))
        def _():
            left_out[half, c] = (own_sum[half, c] + right_in[half, c].astype(F32)).astype(BF16)
            to_left(half, c).start()

    def line_sum(half, c):
        full = own_sum[half, c]
        if n_dp > 1:
            full = full + jnp.where(dp > 0, left_in[half, c].astype(F32), 0.0)
            full = full + jnp.where(dp < n_dp - 1, right_in[half, c].astype(F32), 0.0)
        return full

    half_rows = pd // 2
    loads[0].wait()
    for c in range(3):
        loads[1 + c].wait()
        partial = dot32(embed[...], weights[c])
        for half in range(2):
            piece = partial[half * half_rows : (half + 1) * half_rows]
            own_sum[half, c] = piece
            if half == 0:
                sec_out[0, c] = piece.astype(BF16)
                send_sec(0, c)
            else:
                begin_line(1, c, piece.astype(BF16))

    for load in loads[4:]:
        load.wait()

    first = [jnp.int32(0) for _ in range(clip_count)]
    for f in range(frame_count):
        clip = frame_ref[0, f]
        for c in range(1, clip_count):
            first[c] = first[c] + (clip < c).astype(jnp.int32)
    lengths = [
        (first[c + 1] if c + 1 < clip_count else jnp.int32(frame_count)) - first[c]
        for c in range(clip_count)
    ]
    place_start, place_shift = [], []
    running = jnp.int32(0)
    for r in range(clip_count):
        clip = order_ref[0, r]
        length, start = jnp.int32(0), jnp.int32(0)
        for c in range(clip_count):
            here = clip == c
            length = jnp.where(here, lengths[c], length)
            start = jnp.where(here, first[c], start)
        place_start.append(running)
        place_shift.append(start - running)
        running = running + length

    def clip_at(row):
        clip = jnp.zeros_like(row)
        for c in range(1, clip_count):
            clip = clip + (row >= first[c] * VP).astype(jnp.int32)
        return clip


    @pl.when(me > 0)
    def _():
        rim_copy().wait_recv()

    row = me * rows + lax.broadcasted_iota(jnp.int32, (rows, 1), 0)
    own_clip = clip_at(row)
    summed = None
    for delay in range(taps):
        contrib = dot_t(wide[pl.ds(reach_rows - delay * VP, rows), :], conv[delay])
        if delay:
            before = row - delay * VP
            in_clip = (before >= 0) & (clip_at(before) == own_clip)
            summed = summed + jnp.where(in_clip, contrib, 0.0)
        else:
            summed = contrib
    latents[me] = summed.astype(BF16)
    lat_copies = []
    for d in range(n_tp - 1, 0, -1):
        copy = pltpu.make_async_remote_copy(
            src_ref=latents.at[me], dst_ref=latents.at[me],
            send_sem=lat_send.at[d - 1], recv_sem=lat_recv.at[d - 1],
            device_id={"tp": tp_peers[d - 1]}, device_id_type=MESH,
        )
        copy.start()
        lat_copies.append(copy)

    for c in range(3):
        sum_here = add_sec(0, c)
        own_sum[0, c] = sum_here
        begin_line(0, c, sum_here.astype(BF16))

        @pl.when(2 * dp < n_dp)
        def _():
            pass_right(1, c)

        @pl.when(2 * dp >= n_dp)
        def _():
            pass_left(1, c)

    for c in range(3):
        @pl.when(2 * dp < n_dp)
        def _():
            pass_left(1, c)

        @pl.when(2 * dp >= n_dp)
        def _():
            pass_right(1, c)

        sum_here = line_sum(1, c)
        own_sum[1, c] = sum_here
        sec_out[1, c] = sum_here.astype(BF16)
        send_sec(1, c)

        @pl.when(2 * dp < n_dp)
        def _():
            pass_right(0, c)

        @pl.when(2 * dp >= n_dp)
        def _():
            pass_left(0, c)

    for copy in lat_copies:
        copy.wait_recv()
    latent = latents[...].reshape(total, pd)
    key_row = lax.broadcasted_iota(jnp.int32, (1, total), 1)
    for block in range(n_tp):
        token = block * rows + lax.broadcasted_iota(jnp.int32, (rows, 1), 0)
        shift = jnp.zeros_like(token) + place_shift[0] * VP
        for r in range(1, clip_count):
            shift = jnp.where(token >= place_start[r] * VP, place_shift[r] * VP, shift)
        picks = jnp.where(token + shift == key_row, 1.0, 0.0).astype(BF16)
        packed[pl.ds(block * rows, rows), :] = dot32(picks, latent).astype(BF16)

    def pass_far(c):
        @pl.when(2 * dp < n_dp)
        def _():
            pass_left(0, c)

        @pl.when(2 * dp >= n_dp)
        def _():
            pass_right(0, c)

    at_end = (dp == 0) | (dp == n_dp - 1)

    @pl.when(jnp.logical_not(at_end))
    def _():
        for c in range(3):
            pass_far(c)

    def last_piece(c):
        @pl.when(at_end)
        def _():
            pass_far(c)

    def projected(c):
        last_piece(c)
        full = jnp.concatenate([line_sum(0, c), add_sec(1, c)], axis=0)
        high = full.astype(BF16)
        low = (full - high.astype(F32)).astype(BF16)
        both = dot32(packed[...], jnp.concatenate([high, low], axis=1))
        return both[:, :HD] + both[:, HD:]

    def normed(value, gain):
        scale = lax.rsqrt(jnp.mean(value * value, axis=-1, keepdims=True) + 1e-06)
        return (value * scale * gain).astype(BF16)

    queries[...] = normed(projected(0), gq_ref[...])
    keys[...] = normed(projected(1), gk_ref[...])
    values[...] = projected(2).astype(BF16)

    def place_at(token):
        place = jnp.zeros_like(token)
        for r in range(1, clip_count):
            place = place + (token >= place_start[r] * VP).astype(jnp.int32)
        return place

    key_place = place_at(key_row)

    def attend(blocks):
        query = jnp.concatenate(
            [queries[pl.ds(pl.multiple_of(block * rows, VP), rows), :] for block in blocks], axis=0
        )
        offset = lax.broadcasted_iota(jnp.int32, (rows, 1), 0)
        token = jnp.concatenate([block * rows + offset for block in blocks], axis=0)
        scores = dot_t(query, keys[...])
        scores = jnp.where(place_at(token) == key_place, scores, -1e30)
        highest = jnp.max(scores, axis=-1, keepdims=True)
        expo = jnp.exp((scores - highest) * HD ** (-0.5))
        weight = jnp.sum(expo, axis=-1, keepdims=True)
        return (dot32(expo.astype(BF16), values[...]) / weight).astype(BF16)

    def columns(head):
        return pl.ds(pl.multiple_of(head * HD, HD), HD)

    out_copies = []
    steps = list(range(n_tp - 1, -1, -1))
    for group in [steps[k : k + 2] for k in range(0, n_tp, 2)]:
        result = attend([tp_peers[d - 1] if d else me for d in group])
        for k, d in enumerate(group):
            block_out = result[k * rows : (k + 1) * rows]
            if d == 0:
                out_ref[:, columns(me)] = block_out
                continue
            mixed[d - 1] = block_out
            copy = pltpu.make_async_remote_copy(
                src_ref=mixed.at[d - 1], dst_ref=out_ref.at[:, columns(me)],
                send_sem=out_send.at[d - 1], recv_sem=out_recv.at[d - 1],
                device_id={"tp": tp_peers[d - 1]}, device_id_type=MESH,
            )
            copy.start()
            out_copies.append(copy)

    for copy in lat_copies:
        copy.wait_send()
    for half in range(2):
        for c in range(3):
            for d in range(1, n_sec):
                sec_copy(half, c, d).wait_send()

    @pl.when(me < n_tp - 1)
    def _():
        rim_copy().wait_send()

    @pl.when(dp < n_dp - 1)
    def _():
        for half in range(2):
            for c in range(3):
                to_right(half, c).wait_send()

    @pl.when(dp > 0)
    def _():
        for half in range(2):
            for c in range(3):
                to_left(half, c).wait_send()

    for copy in out_copies:
        copy.wait()


def local(sizes, feats, frame_clip, clip_order, conv_weight, embed_weight, wq, wk, wv, q_gain, k_gain):
    n_sec, n_tp, n_dp = sizes
    feature = feats[0]
    rows, fin = feature.shape
    conv_weight = jnp.swapaxes(conv_weight, 1, 2)
    taps, pd, _ = conv_weight.shape
    depth = wq.shape[0]
    total = rows * n_tp
    direct_embed = depth % 128 == 0
    if not direct_embed:
        slot = lax.axis_index("sec") * n_dp + lax.axis_index("dp")
        embed_weight = lax.dynamic_slice_in_dim(embed_weight, slot * depth, depth, 1)
    hbm, vmem = (pl.BlockSpec(memory_space=space) for space in (pl.ANY, pltpu.VMEM))
    dma = pltpu.SemaphoreType.DMA
    sec_links, tp_links = max(1, n_sec - 1), max(1, n_tp - 1)
    pieces = (2, 3, pd // 2, HD)
    out = pl.pallas_call(
        functools.partial(kernel, sizes, direct_embed),
        out_shape=pltpu.VMEM((rows, n_tp * HD), BF16),
        in_specs=[hbm] * 10,
        out_specs=vmem,
        scratch_shapes=[
            pltpu.VMEM(((taps - 1) * VP + rows, fin), BF16),
            pltpu.VMEM(conv_weight.shape, BF16),
            pltpu.VMEM((pd, depth), BF16),
            pltpu.VMEM((3, depth, HD), BF16),
            pltpu.VMEM(pieces, F32),
            pltpu.VMEM(pieces, BF16),
            pltpu.VMEM((sec_links,) + pieces, BF16),
            pltpu.VMEM(pieces, BF16),
            pltpu.VMEM(pieces, BF16),
            pltpu.VMEM(pieces, BF16),
            pltpu.VMEM(pieces, BF16),
            pltpu.VMEM((n_tp, rows, pd), BF16),
            pltpu.VMEM((total, pd), BF16),
            pltpu.VMEM((total, HD), BF16),
            pltpu.VMEM((total, HD), BF16),
            pltpu.VMEM((total, HD), BF16),
            pltpu.VMEM((tp_links, rows, HD), BF16),
            pltpu.SMEM(frame_clip.shape, jnp.int32),
            pltpu.SMEM(clip_order.shape, jnp.int32),
            pltpu.VMEM(q_gain.shape, F32),
            pltpu.VMEM(k_gain.shape, F32),
            dma((10,)),
            dma(()),
            dma(()),
            dma((sec_links, 2, 3)),
            dma((sec_links, 2, 3)),
            dma((2, 2, 3)),
            dma((2, 2, 3)),
            dma((tp_links,)),
            dma((tp_links,)),
            dma((tp_links,)),
            dma((tp_links,)),
        ],
        compiler_params=pltpu.CompilerParams(collective_id=0, has_side_effects=True),
    )(frame_clip, clip_order, feature, conv_weight, embed_weight, wq, wk, wv, q_gain, k_gain)
    return out[None]


def solution(mesh):
    sizes = tuple(mesh.shape[name] for name in ("sec", "tp", "dp"))
    return jax.shard_map(
        functools.partial(local, sizes),
        mesh=mesh,
        in_specs=(
            P(("sec", "dp"), "tp", None),
            P(("sec", "dp"), None),
            P(("sec", "dp"), None),
            P(),
            P(),
            P(("sec", "dp"), "tp"),
            P(("sec", "dp"), "tp"),
            P(("sec", "dp"), "tp"),
            P("tp", None),
            P("tp", None),
        ),
        out_specs=P(("sec", "dp"), "tp", None),
        check_vma=False,
    )
```
